32 devices in a mesh: ctx: 8 (over z, y), tile: 4 (over x, core).
Axes of the slice: x: 2, y: 2, z: 4, core: 2. Of those that a mesh axis runs over, the one named last changes fastest.
Arguments:
- masks: bfloat16 [16, 512, 512], P('ctx', 'tile'), may hold values from 0 to 1
- blur_rows: bfloat16 [512, 512], replicated, may hold values from -0.25 to 0.25
- blur_cols: bfloat16 [512, 512], replicated, may hold values from -0.25 to 0.25
- pupils: float32 [6, 64, 128], replicated, may hold values from -5 to 5
- targets: bfloat16 [16, 512, 512], P('ctx', 'tile'), may hold values from 0 to 1
- context_masters: int32 [16, 12], P('ctx'), may hold values from 0 to 15, as said below
- offsets: int32 [16, 12, 2], P('ctx'), may hold values from 0 to 511
Outputs:
- resist: bfloat16 [16, 512, 512], P('ctx', 'tile')
- mask_grad: float32 [16, 512, 512], P('ctx', 'tile')
The draws below stay inside these ranges and needn't reach their ends.
Inputs may be any that keep to these rules, and one draw needn't show every extreme that they name: `context_masters`: master m lies on ctx index m // 2. Among the masters named by the 2 contexts of one ctx index there is at most one lying on any one ctx index; a master may be named several times.
All inputs are finite; a program needn't handle non-finite values.
Results may differ from the reference program's by a relative error of at most 0.019.
Values may be sent and summed in bfloat16 or wider, within the bound.
No kernel may reach another device: no remote copies, remote signals or barrier semaphores. Data moves between devices by JAX's collectives and lax.ppermute only.
A program may use at most 64 MiB of HBM per device.

```python
import math
import jax
import jax.numpy as jnp
from jax import lax

PIXELS = 512
MODE_SIDE = 64
KERNELS = 6
MASTER_DEV = 2
CONTEXT_DEV = 2
SOURCES = 12
MASTERS = 16
CONTEXTS = 16


def draw_context_masters(key, part):
    base_key = jax.random.fold_in(key, 7)
    hot_key, jitter_key, choose_key, order_key = jax.random.split(base_key, 4)
    owner_count = MASTERS // MASTER_DEV
    device_count = CONTEXTS // CONTEXT_DEV
    request_count = CONTEXT_DEV * SOURCES
    hotness = jax.random.randint(hot_key, (owner_count,), 0, 4, dtype=jnp.int32)
    jitter = jax.random.randint(jitter_key, (device_count, owner_count), 0, 65536, dtype=jnp.int32)
    scores = (jitter + hotness[None, :] * 65536) * owner_count + jnp.arange(owner_count, dtype=jnp.int32)[None, :]
    ranked = lax.top_k(scores, owner_count)[1].astype(jnp.int32)
    position = jnp.arange(request_count, dtype=jnp.int32) % owner_count
    owners = ranked[:, position]
    shuffle_scores = jax.random.randint(order_key, (device_count, request_count), 0, 65536, dtype=jnp.int32) * request_count + jnp.arange(request_count, dtype=jnp.int32)[None, :]
    shuffle = lax.top_k(shuffle_scores, request_count)[1].astype(jnp.int32)
    owners = jnp.take_along_axis(owners, shuffle, axis=1)
    master_pick = jax.random.randint(choose_key, (device_count, owner_count), 0, MASTER_DEV, dtype=jnp.int32)
    chosen_pick = jnp.take_along_axis(master_pick, owners, axis=1)
    return (owners * MASTER_DEV + chosen_pick).reshape(CONTEXTS, SOURCES).astype(jnp.int32)


def touch_ends(entries, key, smallest, top_value):
    spot = [jax.random.randint(jax.random.fold_in(key, axis), (), 0, length) for axis, length in enumerate(entries.shape)]
    longest = entries.shape.index(max(entries.shape))
    neighbour = spot[:longest] + [(spot[longest] + 1) % entries.shape[longest]] + spot[longest + 1:]
    return entries.at[tuple(spot)].set(smallest).at[tuple(neighbour)].set(top_value)


def block_scale(own_key, dims, cuts, least, largest):
    def one(dim, shards_of):
        heights = jax.random.uniform(jax.random.fold_in(jax.random.fold_in(own_key, 6), dim), (shards_of,), jnp.float32, least / len(cuts), largest / len(cuts))
        return jnp.repeat(jnp.exp(heights), dims[dim] // shards_of).reshape((-1,) + (1,) * (len(dims) - dim - 1))

    factor_of = one(*cuts[0])
    for cut in cuts[1:]:
        factor_of = factor_of * one(*cut)
    return factor_of


def gaussian(own_key, shape, scale, bound, held_as=jnp.bfloat16):
    array = jax.random.normal(own_key, shape, jnp.float32) * scale
    return jnp.minimum(jnp.maximum(array, -bound), bound).astype(held_as)


def setup_inputs(seed: int = 0) -> dict:
    keys = jax.random.split(jax.random.key(seed), 8)
    masks = jnp.clip(1.0 * jax.random.uniform(keys[0], (MASTERS, PIXELS, PIXELS), jnp.float32) ** block_scale(keys[0], (MASTERS, PIXELS, PIXELS), ((0, 8), (1, 4)), -0.2, 0.2), 0.0, 1.0).astype(jnp.bfloat16)
    blur_rows = gaussian(keys[1], (PIXELS, PIXELS), PIXELS ** -0.5, 0.25)
    blur_cols = gaussian(keys[2], (PIXELS, PIXELS), PIXELS ** -0.5, 0.25)
    pupils = gaussian(keys[3], (KERNELS, MODE_SIDE, 2 * MODE_SIDE), 0.8, 5.0, jnp.float32)
    targets = jnp.clip(1.0 * jax.random.uniform(keys[4], (CONTEXTS, PIXELS, PIXELS), jnp.float32) ** block_scale(keys[4], (CONTEXTS, PIXELS, PIXELS), ((0, 8), (1, 4)), -0.2, 0.2), 0.0, 1.0).astype(jnp.bfloat16)
    context_masters = draw_context_masters(jax.random.fold_in(keys[7], 71), 0)
    offsets = touch_ends(jax.random.randint(keys[6], (CONTEXTS, SOURCES, 2), 0, PIXELS), jax.random.fold_in(keys[6], 1), 0, PIXELS - 1).astype(jnp.int32)
    return dict(masks=masks, blur_rows=blur_rows, blur_cols=blur_cols, pupils=pupils, targets=targets, context_masters=context_masters, offsets=offsets)


STEEPNESS = 4.0
THRESHOLD = 1.0

def build_tables(extent, mode_count):
    frequency = (jnp.arange(mode_count, dtype=jnp.int32) - mode_count // 2) % extent
    positions = jnp.arange(extent, dtype=jnp.int32)
    windings = frequency[:, None] * positions[None, :] % extent
    angles = windings.astype(jnp.float32) * (2.0 * math.pi / extent)
    scale_factor = 1.0 / math.sqrt(extent)
    cosine_table = jnp.cos(angles) * scale_factor
    sine_table = jnp.sin(angles) * scale_factor
    row_real = cosine_table.astype(jnp.bfloat16)
    row_imag = (-sine_table).astype(jnp.bfloat16)
    col_fwd = jnp.concatenate([cosine_table.T, -sine_table.T], axis=1).astype(jnp.bfloat16)
    inverse_big = jnp.concatenate([jnp.concatenate([cosine_table, sine_table], axis=1), jnp.concatenate([-sine_table, cosine_table], axis=1)], axis=0).astype(jnp.bfloat16)
    back_real = cosine_table.T.astype(jnp.bfloat16)
    back_imag = sine_table.T.astype(jnp.bfloat16)
    adjoint_big = jnp.concatenate([jnp.concatenate([cosine_table.T, -sine_table.T], axis=1), jnp.concatenate([sine_table.T, cosine_table.T], axis=1)], axis=0).astype(jnp.bfloat16)
    return (row_real, row_imag, col_fwd, inverse_big, back_real, back_imag, adjoint_big)

def complex_left(left_real, left_imag, values):
    width = values.shape[-1] // 2
    real_lead = jnp.einsum('ux,...xv->...uv', left_real.astype(jnp.float32), values.astype(jnp.float32))
    imag_lead = jnp.einsum('ux,...xv->...uv', left_imag.astype(jnp.float32), values.astype(jnp.float32))
    return jnp.concatenate([real_lead[..., :width] - imag_lead[..., width:], real_lead[..., width:] + imag_lead[..., :width]], axis=-1)

def complex_times(factor, values, conjugate):
    width = values.shape[-1] // 2
    factor_real = factor[..., :width]
    factor_imag = factor[..., width:]
    if conjugate:
        factor_imag = -factor_imag
    values_real = values[..., :width]
    values_imag = values[..., width:]
    return jnp.concatenate([factor_real * values_real - factor_imag * values_imag, factor_real * values_imag + factor_imag * values_real], axis=-1)

def phase_table(shifts, row_begin, band_rows, mode_count, extent):
    freq_u = (jnp.arange(band_rows, dtype=jnp.int32) + row_begin - mode_count // 2) % extent
    freq_v = (jnp.arange(mode_count, dtype=jnp.int32) - mode_count // 2) % extent
    windings = (freq_u[None, :, None] * shifts[:, 0][:, None, None] + freq_v[None, None, :] * shifts[:, 1][:, None, None]) % extent
    angles = windings.astype(jnp.float32) * (2.0 * math.pi / extent)
    return jnp.concatenate([jnp.cos(angles), -jnp.sin(angles)], axis=-1)

def image_adjoint(spectrum, target, pupils, back_real, back_imag, row_real, row_imag, inverse_big, adjoint_big):
    amplitude = complex_times(pupils, spectrum[None], False).astype(jnp.bfloat16)
    spread = jnp.einsum('kuv,vy->kuy', amplitude.astype(jnp.float32), inverse_big.astype(jnp.float32)).astype(jnp.bfloat16)
    field = complex_left(back_real, back_imag, spread)
    width = field.shape[-1] // 2
    field_real = field[..., :width]
    field_imag = field[..., width:]
    intensity = lax.optimization_barrier(jnp.sum(field_real * field_real + field_imag * field_imag, axis=0))
    resist = jax.nn.sigmoid(STEEPNESS * (intensity - THRESHOLD))
    slope_term = (resist - target.astype(jnp.float32)) * STEEPNESS * resist * (1.0 - resist)
    pull_back = jnp.concatenate([2.0 * slope_term * field_real, 2.0 * slope_term * field_imag], axis=-1).astype(jnp.bfloat16)
    folded = jnp.einsum('kxy,yv->kxv', pull_back.astype(jnp.float32), adjoint_big.astype(jnp.float32)).astype(jnp.bfloat16)
    grad_amp = complex_left(row_real, row_imag, folded)
    grad_spec = lax.optimization_barrier(jnp.sum(complex_times(pupils, grad_amp, True), axis=0))
    return (resist.astype(jnp.bfloat16), grad_spec)

def reference(masks, blur_rows, blur_cols, pupils, targets, context_masters, offsets):
    extent = masks.shape[1]
    mode_count = pupils.shape[1]
    row_real, row_imag, col_fwd, inverse_big, back_real, back_imag, adjoint_big = build_tables(extent, mode_count)

    def forward(mask):
        half_blur = jnp.dot(mask, blur_cols.T, preferred_element_type=jnp.float32).astype(jnp.bfloat16)
        blurred = jnp.dot(blur_rows, half_blur, preferred_element_type=jnp.float32).astype(jnp.bfloat16)
        column = jnp.dot(blurred, col_fwd, preferred_element_type=jnp.float32).astype(jnp.bfloat16)
        return complex_left(row_real, row_imag, column).astype(jnp.bfloat16)
    spectra = lax.map(forward, masks)
    flat_ids = context_masters.reshape(-1)
    flat_shift = offsets.reshape(-1, 2)
    phases = phase_table(flat_shift, 0, mode_count, mode_count, extent)
    picked = spectra[flat_ids].astype(jnp.float32)
    turned = complex_times(phases, picked, False)
    context_spec = lax.optimization_barrier(jnp.sum(turned.reshape(CONTEXTS, SOURCES, mode_count, 2 * mode_count), axis=1))

    def one_context(inputs):
        spectrum, target = inputs
        return image_adjoint(spectrum, target, pupils, back_real, back_imag, row_real, row_imag, inverse_big, adjoint_big)
    resist, grad_spec = lax.map(one_context, (context_spec, targets))
    back_turn = complex_times(phases, jnp.repeat(grad_spec, SOURCES, axis=0), True)
    master_grad = jax.ops.segment_sum(back_turn, flat_ids, num_segments=MASTERS).astype(jnp.bfloat16)

    def backward(gradient):
        lifted = jnp.dot(gradient, inverse_big, preferred_element_type=jnp.float32).astype(jnp.bfloat16)
        surface = (jnp.dot(back_real, lifted[:, :extent], preferred_element_type=jnp.float32) - jnp.dot(back_imag, lifted[:, extent:], preferred_element_type=jnp.float32)).astype(jnp.bfloat16)
        settled = jnp.dot(surface, blur_cols, preferred_element_type=jnp.float32).astype(jnp.bfloat16)
        return jnp.dot(blur_rows.T, settled, preferred_element_type=jnp.float32)
    mask_grad = lax.map(backward, master_grad)
    return (resist, mask_grad)
```

```python
import functools
import math

import jax
import jax.numpy as jnp
import numpy as np
from jax import lax
from jax.experimental import pallas as pl
from jax.experimental.pallas import tpu as pltpu
from jax.sharding import Mesh
from jax.sharding import PartitionSpec as P

STEEPNESS = 4.0
THRESHOLD = 1.0
BF16 = jnp.bfloat16
F32 = jnp.float32
VMEM_BYTES = 40 << 20


def params(limit=VMEM_BYTES):
    return pltpu.CompilerParams(vmem_limit_bytes=limit)


def vmem_specs(count):
    return [pl.BlockSpec(memory_space=pltpu.VMEM)] * count


def dft_tables(extent, modes):
    frequency = np.arange(modes) - modes // 2
    windings = (frequency[:, None] * np.arange(extent)[None, :]) % extent
    angles = windings.astype(np.float32) * np.float32(2.0 * math.pi / extent)
    scale = 1.0 / math.sqrt(extent)
    cosine = (np.cos(angles) * np.float32(scale)).astype(BF16)
    sine = (np.sin(angles) * np.float32(scale)).astype(BF16)
    forward = np.concatenate([cosine, -sine], axis=0)
    points = np.concatenate([cosine.T, sine.T], axis=1)
    inverse = np.concatenate(
        [np.concatenate([cosine, sine], axis=1), np.concatenate([-sine, cosine], axis=1)], axis=0
    )
    return forward, points, inverse, np.ascontiguousarray(inverse.T)


def dot(a, b):
    return lax.dot_general(a, b, (((1,), (0,)), ((), ())), preferred_element_type=F32)


def dot_nt(a, b):
    return lax.dot_general(a, b, (((1,), (1,)), ((), ())), preferred_element_type=F32)


def dot_tn(a, b):
    return lax.dot_general(a, b, (((0,), (0,)), ((), ())), preferred_element_type=F32)


def left_half(shape):
    return lax.broadcasted_iota(jnp.int32, shape, len(shape) - 1) < shape[-1] // 2


def swap(x):
    return pltpu.roll(x, x.shape[-1] // 2, x.ndim - 1)


def times_i(x):
    turned = swap(x)
    return jnp.where(left_half(x.shape), -turned, turned)


def tile_index(axes):
    return lax.axis_index(axes[0]) * lax.axis_size(axes[1]) + lax.axis_index(axes[1])


def spectrum_kernel(where_ref, masks_ref, br_ref, bc_ref, fwd_ref, keep_ref, send_ref, a_ref, c_ref, full_ref):
    owned, rows, extent = masks_ref.shape
    modes = fwd_ref.shape[0] // 2
    band = modes // 2
    tile_pos = where_ref[0]
    side = where_ref[1]
    own_cols = br_ref[:, pl.ds(pl.multiple_of(tile_pos * rows, rows), rows)]
    c = dot(fwd_ref[...], bc_ref[...]).astype(BF16)
    a = dot(fwd_ref[...], own_cols).astype(BF16)
    c_ref[...] = c
    a_ref[...] = a
    folded = dot_nt(masks_ref[...].reshape(owned * rows, extent), c)
    turned = times_i(folded).astype(BF16)
    folded = folded.astype(BF16)
    for m in range(owned):
        part = slice(m * rows, (m + 1) * rows)
        full_ref[m] = dot(a[:modes], folded[part]) + dot(a[modes:], turned[part])
    keep_ref[...] = full_ref[:, pl.ds(pl.multiple_of(side * band, band), band), :]
    send_ref[...] = full_ref[:, pl.ds(pl.multiple_of((1 - side) * band, band), band), :]


def phase_kernel(where_ref, masters_ref, offsets_ref, w1_ref, w2_ref, *, sources, extent):
    contexts, masters, band, width = w1_ref.shape
    modes = width // 2
    side = where_ref[1]
    w1_ref[...] = jnp.zeros_like(w1_ref)
    w2_ref[...] = jnp.zeros_like(w2_ref)
    count = contexts * sources
    step = 2.0 * math.pi / extent
    freq_u = lax.broadcasted_iota(jnp.int32, (band, 128), 0) + side * band - modes // 2
    lane = lax.broadcasted_iota(jnp.int32, (1, 128), 1)
    row = lax.broadcasted_iota(jnp.int32, (count, 1), 0)
    shift_r = jnp.zeros((1, 128), jnp.int32)
    shift_s = jnp.zeros((count, 1), jnp.int32)
    for j in range(count):
        shift_r = jnp.where(lane == j, offsets_ref[2 * j], shift_r)
        shift_s = jnp.where(row == j, offsets_ref[2 * j + 1], shift_s)
    angle_u = ((freq_u * shift_r) & (extent - 1)).astype(F32) * step
    lanes = lax.broadcasted_iota(jnp.int32, (count, width), 1)
    freq_v = (lanes & (modes - 1)) - modes // 2
    angle_v = ((freq_v * shift_s) & (extent - 1)).astype(F32) * step
    p_re, p_im = jnp.cos(angle_u), -jnp.sin(angle_u)
    q_re, q_im = jnp.cos(angle_v), -jnp.sin(angle_v)
    left = left_half((count, width))
    signed_im = jnp.where(left, q_im, -q_im)
    signed_re = jnp.where(left, q_re, -q_re)
    for c in range(contexts):
        for j in range(sources):
            i = c * sources + j
            m = masters_ref[i]
            re = jnp.broadcast_to(p_re[:, i : i + 1], (band, width))
            im = jnp.broadcast_to(p_im[:, i : i + 1], (band, width))
            one = slice(i, i + 1)
            w1_ref[c, m] = w1_ref[c, m] + re * q_re[one] - im * q_im[one]
            w2_ref[c, m] = w2_ref[c, m] + re * signed_im[one] + im * signed_re[one]


def over_masters(count, body, init):
    if count <= 16:
        for i in range(count):
            init = body(i, init)
        return init
    return lax.fori_loop(0, count, body, init)


def context_kernel(got_ref, w1_ref, w2_ref, spec_ref):
    owners, halves, owned, band, width = got_ref.shape
    contexts = w1_ref.shape[0]

    def body(d, sums):
        sums = list(sums)
        for m in range(owned):
            value = got_ref[d, 0, m].astype(F32)
            for h in range(1, halves):
                value = value + got_ref[d, h, m].astype(F32)
            for c in range(contexts):
                sums[2 * c] = sums[2 * c] + value * w1_ref[c, d * owned + m]
                sums[2 * c + 1] = sums[2 * c + 1] + value * w2_ref[c, d * owned + m]
        return tuple(sums)

    zero = jnp.zeros((band, width), F32)
    sums = over_masters(owners, body, (zero,) * (2 * contexts))
    for c in range(contexts):
        spec_ref[c] = sums[2 * c] + swap(sums[2 * c + 1])


def join_bands(full_ref, side, mine, other):
    band = mine.shape[-2]
    full_ref[:, pl.ds(pl.multiple_of(side * band, band), band), :] = mine
    full_ref[:, pl.ds(pl.multiple_of((1 - side) * band, band), band), :] = other


def image_kernel(
    where_ref, mine_ref, other_ref, pupils_ref, targets_ref, fwd_ref, points_ref, inv_ref, adj_ref,
    resist_ref, keep_ref, send_ref,
    spec_ref, left_ref, field_ref, pull_ref,
):
    kernels, modes, width = pupils_ref.shape
    contexts, rows, extent = targets_ref.shape
    band = modes // 2
    tile_pos = where_ref[0]
    side = where_ref[1]
    join_bands(spec_ref, side, mine_ref[...], other_ref[...])
    own = pl.ds(pl.multiple_of(tile_pos * rows, rows), rows)
    points = points_ref[own, :]
    own_fwd = jnp.concatenate([fwd_ref[:modes, own], fwd_ref[modes:, own]], axis=1)
    left = left_half((modes, width))

    def pupil_parts(k):
        pupil = pupils_ref[k]
        turned = swap(pupil)
        return jnp.where(left, pupil, turned), jnp.where(left, -turned, pupil)

    block = 16

    def one_context(c, carry):
        spec = spec_ref[c]
        spec_turned = swap(spec)
        for k in range(kernels):
            same, cross = pupil_parts(k)
            amp = spec * same + spec_turned * cross
            stack = jnp.concatenate([amp.astype(BF16), times_i(amp).astype(BF16)], axis=0)
            left_ref[k * rows : (k + 1) * rows, :] = dot(points, stack).astype(BF16)
        field_ref[...] = dot(left_ref[...], inv_ref[...])

        def one_block(b, carry):
            begin = pl.multiple_of(b * block, block)
            intensity = jnp.zeros((block, extent), F32)
            for k in range(kernels):
                re = field_ref[pl.ds(k * rows + begin, block), :extent]
                im = field_ref[pl.ds(k * rows + begin, block), extent:]
                intensity = intensity + re * re + im * im
            resist = jax.nn.sigmoid(STEEPNESS * (intensity - THRESHOLD))
            target = targets_ref[c, pl.ds(begin, block), :].astype(F32)
            slope = (resist - target) * (2.0 * STEEPNESS) * resist * (1.0 - resist)
            resist_ref[c, pl.ds(begin, block), :] = resist.astype(BF16)
            for k in range(kernels):
                at = pl.ds(k * rows + begin, block)
                pull_ref[at, :extent] = (slope * field_ref[at, :extent]).astype(BF16)
                pull_ref[at, extent:] = (slope * field_ref[at, extent:]).astype(BF16)
            return carry

        lax.fori_loop(0, rows // block, one_block, 0)
        folded = dot(pull_ref[...], adj_ref[...])
        total = jnp.zeros((modes, width), F32)
        for k in range(kernels):
            same, cross = pupil_parts(k)
            part = folded[k * rows : (k + 1) * rows]
            stack = jnp.concatenate([part.astype(BF16), times_i(part).astype(BF16)], axis=0)
            grad = dot(own_fwd, stack)
            total = total + grad * same - swap(grad) * cross
        spec_ref[c] = total
        return carry

    lax.fori_loop(0, contexts, one_context, 0)
    keep_ref[...] = spec_ref[:, pl.ds(pl.multiple_of(side * band, band), band), :]
    send_ref[...] = spec_ref[:, pl.ds(pl.multiple_of((1 - side) * band, band), band), :]


def scatter_kernel(mine_ref, other_ref, w1_ref, w2_ref, out_ref):
    owners, halves, owned, band, width = out_ref.shape
    contexts = w1_ref.shape[0]
    grads = [mine_ref[c] + other_ref[c] for c in range(contexts)]
    turned = [swap(grad) for grad in grads]

    def body(d, carry):
        for m in range(owned):
            value = jnp.zeros((band, width), F32)
            for c in range(contexts):
                value = value + grads[c] * w1_ref[c, d * owned + m] + turned[c] * w2_ref[c, d * owned + m]
            value = value.astype(BF16)
            for h in range(halves):
                out_ref[d, h, m] = value
        return carry

    over_masters(owners, body, 0)


def gather_kernel(got_ref, out_ref):
    owners, halves, owned, band, width = got_ref.shape

    def body(d, sums):
        return tuple(
            sum((got_ref[d, h, m].astype(F32) for h in range(halves)), sums[m]) for m in range(owned)
        )

    sums = over_masters(owners, body, (jnp.zeros((band, width), F32),) * owned)
    for m in range(owned):
        out_ref[m] = sums[m].astype(out_ref.dtype)


def lift_kernel(where_ref, mine_ref, other_ref, a_ref, c_ref, out_ref, full_ref):
    owned = out_ref.shape[0]
    side = where_ref[1]
    join_bands(full_ref, side, mine_ref[...], other_ref[...])
    for m in range(owned):
        grad = full_ref[m]
        stack = jnp.concatenate([grad.astype(BF16), (-times_i(grad)).astype(BF16)], axis=0)
        lifted = dot_tn(a_ref[...], stack).astype(BF16)
        out_ref[m] = dot(lifted, c_ref[...])


def local(masks, blur_rows, blur_cols, pupils, targets, context_masters, offsets):
    owned, rows, extent = masks.shape
    kernels, modes, width = pupils.shape
    contexts, sources = context_masters.shape
    owners = lax.axis_size("ctx")
    halves = lax.axis_size("hi")
    band = modes // 2
    masters = owners * owned
    tables = dft_tables(extent, modes)
    forward, points, inverse, adjoint = (jnp.asarray(table) for table in tables)
    where = jnp.stack([tile_index(("hi", "lo")), lax.axis_index("lo")]).astype(jnp.int32)
    smem = pl.BlockSpec(memory_space=pltpu.SMEM)
    vmem = pl.BlockSpec(memory_space=pltpu.VMEM)
    band_f32 = jax.ShapeDtypeStruct((owned, band, width), F32)
    ctx_f32 = jax.ShapeDtypeStruct((contexts, band, width), F32)

    def swap_sides(x):
        return lax.ppermute(x, "lo", [(0, 1), (1, 0)])

    def exchange(x):
        flat = x.reshape((owners * halves,) + x.shape[2:])
        got = lax.all_to_all(flat, ("ctx", "hi"), split_axis=0, concat_axis=0, tiled=True)
        return got.reshape(x.shape)

    keep, send, a_table, c_table = pl.pallas_call(
        spectrum_kernel,
        out_shape=(
            band_f32,
            band_f32,
            jax.ShapeDtypeStruct((width, rows), BF16),
            jax.ShapeDtypeStruct((width, extent), BF16),
        ),
        in_specs=[smem] + [vmem] * 4,
        out_specs=(vmem,) * 4,
        scratch_shapes=[pltpu.VMEM((owned, modes, width), F32)],
        compiler_params=params(),
        cost_estimate=pl.CostEstimate(flops=400_000_000, bytes_accessed=2_000_000, transcendentals=0),
    )(where, masks, blur_rows, blur_cols, forward)
    spectra = (keep + swap_sides(send)).astype(BF16)
    outgoing = jnp.broadcast_to(spectra[None, None], (owners, halves, owned, band, width))
    incoming = exchange(outgoing)

    w_shape = jax.ShapeDtypeStruct((contexts, masters, band, width), F32)
    w1, w2 = pl.pallas_call(
        functools.partial(phase_kernel, sources=sources, extent=extent),
        out_shape=(w_shape, w_shape),
        in_specs=[smem] * 3,
        out_specs=(vmem,) * 2,
        compiler_params=params(),
        cost_estimate=pl.CostEstimate(flops=100_000_000, bytes_accessed=1_000_000, transcendentals=0),
    )(where, context_masters.reshape(-1), offsets.reshape(-1))

    spec = pl.pallas_call(
        context_kernel,
        out_shape=ctx_f32,
        in_specs=[vmem] * 3,
        out_specs=vmem,
        compiler_params=params(),
        cost_estimate=pl.CostEstimate(flops=10_000_000, bytes_accessed=1_000_000, transcendentals=0),
    )(incoming, w1, w2)

    resist, keep, send = pl.pallas_call(
        image_kernel,
        out_shape=(jax.ShapeDtypeStruct((contexts, rows, extent), BF16), ctx_f32, ctx_f32),
        in_specs=[smem] + [vmem] * 8,
        out_specs=(vmem,) * 3,
        scratch_shapes=[
            pltpu.VMEM((contexts, modes, width), F32),
            pltpu.VMEM((kernels * rows, width), BF16),
            pltpu.VMEM((kernels * rows, 2 * extent), F32),
            pltpu.VMEM((kernels * rows, 2 * extent), BF16),
        ],
        compiler_params=params(),
        cost_estimate=pl.CostEstimate(flops=2_000_000_000, bytes_accessed=2_000_000, transcendentals=0),
    )(where, spec, swap_sides(spec), pupils, targets, forward, points, inverse, adjoint)

    returned = pl.pallas_call(
        scatter_kernel,
        out_shape=jax.ShapeDtypeStruct((owners, halves, owned, band, width), BF16),
        in_specs=[vmem] * 4,
        out_specs=vmem,
        compiler_params=params(),
        cost_estimate=pl.CostEstimate(flops=10_000_000, bytes_accessed=1_000_000, transcendentals=0),
    )(keep, swap_sides(send), w1, w2)
    arrived = exchange(returned)
    master_grad = pl.pallas_call(
        gather_kernel,
        out_shape=band_f32,
        in_specs=[vmem],
        out_specs=vmem,
        compiler_params=params(),
        cost_estimate=pl.CostEstimate(flops=10_000_000, bytes_accessed=1_000_000, transcendentals=0),
    )(arrived)
    mask_grad = pl.pallas_call(
        lift_kernel,
        out_shape=jax.ShapeDtypeStruct((owned, rows, extent), F32),
        in_specs=[smem] + [vmem] * 4,
        out_specs=vmem,
        scratch_shapes=[pltpu.VMEM((owned, modes, width), F32)],
        compiler_params=params(),
        cost_estimate=pl.CostEstimate(flops=100_000_000, bytes_accessed=1_000_000, transcendentals=0),
    )(where, master_grad, swap_sides(master_grad), a_table, c_table)
    return resist, mask_grad


def solution(mesh):
    devices = mesh.devices
    contexts, tiles = devices.shape
    fine = Mesh(devices.reshape(contexts, tiles // 2, 2), ("ctx", "hi", "lo"))
    rows = ("hi", "lo")
    placed = (
        P("ctx", rows, None),
        P(),
        P(),
        P(),
        P("ctx", rows, None),
        P("ctx", None),
        P("ctx", None, None),
    )
    return jax.shard_map(
        local,
        mesh=fine,
        in_specs=placed,
        out_specs=(P("ctx", rows, None), P("ctx", rows, None)),
        check_vma=False,
    )
```

```python
import functools
import math

import jax
import jax.numpy as jnp
import numpy as np
from jax import lax
from jax.experimental import pallas as pl
from jax.experimental.pallas import tpu as pltpu
from jax.sharding import Mesh
from jax.sharding import PartitionSpec as P


STEEPNESS = 4.0
THRESHOLD = 1.0
BF16 = jnp.bfloat16
F32 = jnp.float32
VMEM_BYTES = 40 << 20


def params(limit=VMEM_BYTES):
    return pltpu.CompilerParams(vmem_limit_bytes=limit)


def dft_tables(extent, modes):
    frequency = np.arange(modes) - modes // 2
    windings = (frequency[:, None] * np.arange(extent)[None, :]) % extent
    angles = windings.astype(np.float32) * np.float32(2.0 * math.pi / extent)
    scale = 1.0 / math.sqrt(extent)
    cosine = (np.cos(angles) * np.float32(scale)).astype(BF16)
    sine = (np.sin(angles) * np.float32(scale)).astype(BF16)
    forward = np.concatenate([cosine, -sine], axis=0)
    points = np.concatenate([cosine.T, sine.T], axis=1)
    inverse = np.concatenate(
        [np.concatenate([cosine, sine], axis=1), np.concatenate([-sine, cosine], axis=1)], axis=0
    )
    return forward, points, inverse, np.ascontiguousarray(inverse.T)


def dot(a, b):
    return lax.dot_general(a, b, (((1,), (0,)), ((), ())), preferred_element_type=F32)


def dot_nt(a, b):
    return lax.dot_general(a, b, (((1,), (1,)), ((), ())), preferred_element_type=F32)


def dot_tn(a, b):
    return lax.dot_general(a, b, (((0,), (0,)), ((), ())), preferred_element_type=F32)


def left_half(shape):
    return lax.broadcasted_iota(jnp.int32, shape, len(shape) - 1) < shape[-1] // 2


def swap(x):
    return pltpu.roll(x, x.shape[-1] // 2, x.ndim - 1)


def times_i(x):
    turned = swap(x)
    return jnp.where(left_half(x.shape), -turned, turned)


def tile_index():
    return lax.axis_index("hi") * lax.axis_size("lo") + lax.axis_index("lo")


def spectrum_kernel(
    masks_hbm, br_hbm, bc_hbm, fwd_hbm,
    keep_ref, send_ref, a_ref, c_ref,
    full_ref, masks_ref, br_ref, bc_ref, fwd_ref, sems,
):
    owned, rows, extent = masks_ref.shape
    modes = fwd_ref.shape[0] // 2
    band = modes // 2
    side = lax.axis_index("lo")
    own = pl.ds(pl.multiple_of(tile_index() * rows, rows), rows)
    loads = [
        pltpu.make_async_copy(fwd_hbm, fwd_ref, sems.at[0]),
        pltpu.make_async_copy(bc_hbm, bc_ref, sems.at[1]),
        pltpu.make_async_copy(masks_hbm, masks_ref, sems.at[2]),
        pltpu.make_async_copy(br_hbm.at[:, own], br_ref, sems.at[3]),
    ]
    for load in loads:
        load.start()
    loads[0].wait()
    loads[1].wait()
    c = dot(fwd_ref[...], bc_ref[...]).astype(BF16)
    c_ref[...] = c
    loads[3].wait()
    a = dot(fwd_ref[...], br_ref[...]).astype(BF16)
    a_ref[...] = a
    loads[2].wait()
    folded = dot_nt(masks_ref[...].reshape(owned * rows, extent), c)
    turned = times_i(folded).astype(BF16)
    folded = folded.astype(BF16)
    for m in range(owned):
        part = slice(m * rows, (m + 1) * rows)
        full_ref[m] = dot(a[:modes], folded[part]) + dot(a[modes:], turned[part])
    keep_ref[...] = full_ref[:, pl.ds(pl.multiple_of(side * band, band), band), :]
    send_ref[...] = full_ref[:, pl.ds(pl.multiple_of((1 - side) * band, band), band), :]


def spread_kernel(mine_ref, other_ref, out_ref):
    owners, halves = out_ref.shape[:2]
    value = (mine_ref[...] + other_ref[...]).astype(BF16)
    for d in range(owners):
        for h in range(halves):
            out_ref[d, h] = value


def phase_kernel(masters_ref, offsets_ref, w1_ref, w2_ref, named_ref, *, extent):
    contexts, masters, band, width = w1_ref.shape
    sources = masters_ref.shape[1]
    owned = masters // named_ref.shape[0]
    modes = width // 2
    side = lax.axis_index("lo")
    named_ref[...] = jnp.zeros_like(named_ref)
    w1_ref[...] = jnp.zeros_like(w1_ref)
    w2_ref[...] = jnp.zeros_like(w2_ref)
    count = contexts * sources
    step = 2.0 * math.pi / extent
    freq_u = lax.broadcasted_iota(jnp.int32, (band, 128), 0) + side * band - modes // 2
    lane = lax.broadcasted_iota(jnp.int32, (1, 128), 1)
    row = lax.broadcasted_iota(jnp.int32, (count, 1), 0)
    shift_r = jnp.zeros((1, 128), jnp.int32)
    shift_s = jnp.zeros((count, 1), jnp.int32)
    for j in range(count):
        shift_r = jnp.where(lane == j, offsets_ref[j // sources, 0, j % sources], shift_r)
        shift_s = jnp.where(row == j, offsets_ref[j // sources, 1, j % sources], shift_s)
    angle_u = ((freq_u * shift_r) & (extent - 1)).astype(F32) * step
    lanes = lax.broadcasted_iota(jnp.int32, (count, width), 1)
    freq_v = (lanes & (modes - 1)) - modes // 2
    angle_v = ((freq_v * shift_s) & (extent - 1)).astype(F32) * step
    p_re, p_im = jnp.cos(angle_u), -jnp.sin(angle_u)
    q_re, q_im = jnp.cos(angle_v), -jnp.sin(angle_v)
    left = left_half((count, width))
    signed_im = jnp.where(left, q_im, -q_im)
    signed_re = jnp.where(left, q_re, -q_re)
    for c in range(contexts):
        for j in range(sources):
            i = c * sources + j
            m = masters_ref[c, j]
            named_ref[m // owned, pl.ds(m % owned, 1), :] = jnp.ones((1, width), F32)
            re = jnp.broadcast_to(p_re[:, i : i + 1], (band, width))
            im = jnp.broadcast_to(p_im[:, i : i + 1], (band, width))
            one = slice(i, i + 1)
            w1_ref[c, m] = w1_ref[c, m] + re * q_re[one] - im * q_im[one]
            w2_ref[c, m] = w2_ref[c, m] + re * signed_im[one] + im * signed_re[one]


def over_masters(count, body, init):
    if count <= 16:
        for i in range(count):
            init = body(i, init)
        return init
    return lax.fori_loop(0, count, body, init)


def context_kernel(got_ref, w1_ref, w2_ref, spec_ref):
    owners, halves, owned, band, width = got_ref.shape
    contexts = w1_ref.shape[0]

    def body(d, sums):
        sums = list(sums)
        for m in range(owned):
            value = got_ref[d, 0, m].astype(F32)
            for h in range(1, halves):
                value = value + got_ref[d, h, m].astype(F32)
            for c in range(contexts):
                sums[2 * c] = sums[2 * c] + value * w1_ref[c, d * owned + m]
                sums[2 * c + 1] = sums[2 * c + 1] + value * w2_ref[c, d * owned + m]
        return tuple(sums)

    zero = jnp.zeros((band, width), F32)
    sums = over_masters(owners, body, (zero,) * (2 * contexts))
    for c in range(contexts):
        spec_ref[c] = sums[2 * c] + swap(sums[2 * c + 1])


def join_bands(full_ref, side, mine, other):
    band = mine.shape[-2]
    full_ref[:, pl.ds(pl.multiple_of(side * band, band), band), :] = mine
    full_ref[:, pl.ds(pl.multiple_of((1 - side) * band, band), band), :] = other


def image_kernel(
    mine_ref, other_ref, pupils_ref, targets_ref, fwd_ref, points_ref, inv_ref, adj_ref,
    resist_ref, keep_ref, send_ref,
    spec_ref, left_ref, field_ref, pull_ref,
):
    kernels, modes, width = pupils_ref.shape
    contexts, rows, extent = targets_ref.shape
    band = modes // 2
    tile_pos = tile_index()
    side = lax.axis_index("lo")
    join_bands(spec_ref, side, mine_ref[...], other_ref[...])
    own = pl.ds(pl.multiple_of(tile_pos * rows, rows), rows)
    points = points_ref[own, :]
    own_fwd = jnp.concatenate([fwd_ref[:modes, own], fwd_ref[modes:, own]], axis=1)
    left = left_half((modes, width))

    def pupil_parts(k):
        pupil = pupils_ref[k]
        turned = swap(pupil)
        return jnp.where(left, pupil, turned), jnp.where(left, -turned, pupil)

    block = 16

    def one_context(c, carry):
        spec = spec_ref[c]
        spec_turned = swap(spec)
        for k in range(kernels):
            same, cross = pupil_parts(k)
            amp = spec * same + spec_turned * cross
            stack = jnp.concatenate([amp.astype(BF16), times_i(amp).astype(BF16)], axis=0)
            left_ref[k * rows : (k + 1) * rows, :] = dot(points, stack).astype(BF16)
        field_ref[...] = dot(left_ref[...], inv_ref[...])

        def one_block(b, carry):
            begin = pl.multiple_of(b * block, block)
            intensity = jnp.zeros((block, extent), F32)
            for k in range(kernels):
                re = field_ref[pl.ds(k * rows + begin, block), :extent]
                im = field_ref[pl.ds(k * rows + begin, block), extent:]
                intensity = intensity + re * re + im * im
            resist = jax.nn.sigmoid(STEEPNESS * (intensity - THRESHOLD))
            target = targets_ref[c, pl.ds(begin, block), :].astype(F32)
            slope = (resist - target) * (2.0 * STEEPNESS) * resist * (1.0 - resist)
            resist_ref[c, pl.ds(begin, block), :] = resist.astype(BF16)
            for k in range(kernels):
                at = pl.ds(k * rows + begin, block)
                pull_ref[at, :extent] = (slope * field_ref[at, :extent]).astype(BF16)
                pull_ref[at, extent:] = (slope * field_ref[at, extent:]).astype(BF16)
            return carry

        lax.fori_loop(0, rows // block, one_block, 0)
        folded = dot(pull_ref[...], adj_ref[...])
        total = jnp.zeros((modes, width), F32)
        for k in range(kernels):
            same, cross = pupil_parts(k)
            part = folded[k * rows : (k + 1) * rows]
            stack = jnp.concatenate([part.astype(BF16), times_i(part).astype(BF16)], axis=0)
            grad = dot(own_fwd, stack)
            total = total + grad * same - swap(grad) * cross
        spec_ref[c] = total
        return carry

    lax.fori_loop(0, contexts, one_context, 0)
    keep_ref[...] = spec_ref[:, pl.ds(pl.multiple_of(side * band, band), band), :]
    send_ref[...] = spec_ref[:, pl.ds(pl.multiple_of((1 - side) * band, band), band), :]


def scatter_kernel(mine_ref, other_ref, w1_ref, w2_ref, named_ref, out_ref):
    owners, halves, _, width = out_ref.shape
    contexts, masters, band, _ = w1_ref.shape
    owned = masters // owners
    grads = [mine_ref[c] + other_ref[c] for c in range(contexts)]
    turned = [swap(grad) for grad in grads]

    def body(d, carry):
        value = jnp.zeros((band, width), F32)
        for m in range(owned):
            for c in range(contexts):
                value = value + grads[c] * w1_ref[c, d * owned + m] + turned[c] * w2_ref[c, d * owned + m]
        value = value.astype(BF16)
        named = named_ref[d].astype(BF16)
        for h in range(halves):
            out_ref[d, h, :band] = value
            out_ref[d, h, band:] = named
        return carry

    over_masters(owners, body, 0)


def gather_kernel(got_ref, out_ref):
    owners, halves, _, width = got_ref.shape
    owned, band, _ = out_ref.shape

    def body(d, sums):
        value = sum(got_ref[d, h, :band].astype(F32) for h in range(halves))
        named = got_ref[d, 0, band:].astype(F32)
        return tuple(sums[m] + value * named[m : m + 1] for m in range(owned))

    sums = over_masters(owners, body, (jnp.zeros((band, width), F32),) * owned)
    for m in range(owned):
        out_ref[m] = sums[m]


def lift_kernel(mine_ref, other_ref, a_ref, c_ref, out_ref, full_ref):
    owned = out_ref.shape[0]
    side = lax.axis_index("lo")
    join_bands(full_ref, side, mine_ref[...], other_ref[...])
    for m in range(owned):
        grad = full_ref[m]
        stack = jnp.concatenate([grad.astype(BF16), (-times_i(grad)).astype(BF16)], axis=0)
        lifted = dot_tn(a_ref[...], stack).astype(BF16)
        out_ref[m] = dot(lifted, c_ref[...])


def local(masks, blur_rows, blur_cols, pupils, targets, context_masters, offsets):
    owned, rows, extent = masks.shape
    kernels, modes, width = pupils.shape
    contexts, _ = context_masters.shape
    owners = lax.axis_size("ctx")
    halves = lax.axis_size("hi")
    band = modes // 2
    masters = owners * owned
    forward, points, inverse, adjoint = (jnp.asarray(t) for t in dft_tables(extent, modes))
    flag_rows = 8 * pl.cdiv(owned, 8)
    smem = pl.BlockSpec(memory_space=pltpu.SMEM)
    vmem = pl.BlockSpec(memory_space=pltpu.VMEM)
    hbm = pl.BlockSpec(memory_space=pltpu.HBM)
    band_f32 = jax.ShapeDtypeStruct((owned, band, width), F32)
    ctx_f32 = jax.ShapeDtypeStruct((contexts, band, width), F32)

    def swap_sides(x):
        return lax.ppermute(x, "lo", [(0, 1), (1, 0)])

    def exchange(x):
        flat = x.reshape((owners * halves,) + x.shape[2:])
        got = lax.all_to_all(flat, ("ctx", "hi"), split_axis=0, concat_axis=0, tiled=True)
        return got.reshape(x.shape)

    def call(kernel, out_shape, in_specs, *args, scratch=(), flops=1_000_000, limit=VMEM_BYTES):
        return pl.pallas_call(
            kernel,
            out_shape=out_shape,
            in_specs=in_specs,
            out_specs=jax.tree.map(lambda _: vmem, out_shape),
            scratch_shapes=scratch,
            compiler_params=params(limit),
            cost_estimate=pl.CostEstimate(flops=flops, bytes_accessed=1_000_000, transcendentals=0),
        )(*args)

    keep, send, a_table, c_table = call(
        spectrum_kernel,
        (
            band_f32,
            band_f32,
            jax.ShapeDtypeStruct((width, rows), BF16),
            jax.ShapeDtypeStruct((width, extent), BF16),
        ),
        [hbm] * 4,
        *(pltpu.with_memory_space_constraint(x, pltpu.HBM) for x in (masks, blur_rows, blur_cols, forward)),
        scratch=[
            pltpu.VMEM((owned, modes, width), F32),
            pltpu.VMEM((owned, rows, extent), BF16),
            pltpu.VMEM((extent, rows), BF16),
            pltpu.VMEM((extent, extent), BF16),
            pltpu.VMEM((width, extent), BF16),
            pltpu.SemaphoreType.DMA((4,)),
        ],
        flops=400_000_000,
    )
    other = swap_sides(send)
    w_shape = jax.ShapeDtypeStruct((contexts, masters, band, width), F32)
    w1, w2, named = call(
        functools.partial(phase_kernel, extent=extent),
        (w_shape, w_shape, jax.ShapeDtypeStruct((owners, flag_rows, width), F32)),
        [smem] * 2,
        context_masters,
        jnp.swapaxes(offsets, 1, 2),
        flops=100_000_000,
    )
    outgoing = call(
        spread_kernel,
        jax.ShapeDtypeStruct((owners, halves, owned, band, width), BF16),
        [vmem] * 2,
        keep,
        other,
    )
    spec = call(context_kernel, ctx_f32, [vmem] * 3, exchange(outgoing), w1, w2)
    resist, keep, send = call(
        image_kernel,
        (jax.ShapeDtypeStruct((contexts, rows, extent), BF16), ctx_f32, ctx_f32),
        [vmem] * 8,
        spec,
        swap_sides(spec),
        pupils,
        targets,
        forward,
        points,
        inverse,
        adjoint,
        scratch=[
            pltpu.VMEM((contexts, modes, width), F32),
            pltpu.VMEM((kernels * rows, width), BF16),
            pltpu.VMEM((kernels * rows, 2 * extent), F32),
            pltpu.VMEM((kernels * rows, 2 * extent), BF16),
        ],
        flops=2_000_000_000,
    )
    returned = call(
        scatter_kernel,
        jax.ShapeDtypeStruct((owners, halves, band + flag_rows, width), BF16),
        [vmem] * 5,
        keep,
        swap_sides(send),
        w1,
        w2,
        named,
    )
    master_grad = call(gather_kernel, band_f32, [vmem], exchange(returned))
    mask_grad = call(
        lift_kernel,
        jax.ShapeDtypeStruct((owned, rows, extent), F32),
        [vmem] * 4,
        master_grad,
        swap_sides(master_grad),
        a_table,
        c_table,
        scratch=[pltpu.VMEM((owned, modes, width), F32)],
        flops=100_000_000,
    )
    return resist, mask_grad


def solution(mesh):
    devices = mesh.devices
    contexts, tiles = devices.shape
    fine = Mesh(devices.reshape(contexts, tiles // 2, 2), ("ctx", "hi", "lo"))
    rows = ("hi", "lo")
    placed = (
        P("ctx", rows, None),
        P(),
        P(),
        P(),
        P("ctx", rows, None),
        P("ctx", None),
        P("ctx", None, None),
    )
    return jax.shard_map(
        local,
        mesh=fine,
        in_specs=placed,
        out_specs=(P("ctx", rows, None), P("ctx", rows, None)),
        check_vma=False,
    )
```
